128 devices in a mesh: row: 16 (over z, x), col: 8 (over y, core).
Axes of the slice: x: 4, y: 4, z: 4, core: 2. Of those that a mesh axis runs over, the one named last changes fastest.
Arguments:
- panel: float32 [16, 8192, 8, 512], P('row', None, 'col'), may hold values from -1 to 4, as said below
- rhs: float32 [16, 8192, 256], P('row'), may hold values from -6 to 6
Outputs:
- solved: float32 [8, 512, 256], P('col')
- remainder: float32 [16, 8192, 256], P('row', None, 'col')
The draws below stay inside these ranges and needn't reach their ends.
Inputs may be any that keep to these rules, and one draw needn't show every extreme that they name: panel is lower triangular in the global indices: entries with column above row are zero, diagonal entries lie between 2 and 4, the others are of size about 1 / sqrt(4096).
All inputs are finite; a program needn't handle non-finite values.
Results may differ from the reference program's by a relative error of at most 0.000084.
Values sent between devices are 32-bit elements; how exact they have to be, the bound alone decides.
A program may use at most 192 MiB of HBM per device.

```python
import math
import jax
import jax.numpy as jnp
from jax import lax

ORDER = 131072
TB = 512
STEPS = 8
RHS = 256
ROW_CLASSES = 16
COL_CLASSES = 8
RT_DEV = 16
CT_DEV = 1


def draw_panel(key, part):
    array_shape = (ROW_CLASSES, RT_DEV * TB, COL_CLASSES, CT_DEV * TB)
    row_class = lax.broadcasted_iota(jnp.int32, array_shape, 0)
    row_inner = lax.broadcasted_iota(jnp.int32, array_shape, 1)
    col_class = lax.broadcasted_iota(jnp.int32, array_shape, 2)
    col_inner = lax.broadcasted_iota(jnp.int32, array_shape, 3)
    global_row = (row_inner // TB * ROW_CLASSES + row_class) * TB + row_inner % TB
    global_col = (col_inner // TB * COL_CLASSES + col_class) * TB + col_inner % TB
    key_off = jax.random.fold_in(key, 11)
    key_diag = jax.random.fold_in(key, 23)
    off_diag = jnp.clip(jax.random.normal(key_off, array_shape, jnp.float32), -6.0, 6.0)
    same_tile = (global_row // TB == global_col // TB).astype(jnp.float32)
    below_tile = (global_row // TB == global_col // TB + 1).astype(jnp.float32)
    off_diag = (off_diag + 0.3 * same_tile + 0.45 * below_tile) / math.sqrt(STEPS * TB)
    diag_vals = jax.random.uniform(key_diag, array_shape, jnp.float32, 2.0, 4.0)
    entries = jnp.where(global_col > global_row, 0.0, jnp.where(global_col == global_row, diag_vals, off_diag))
    return entries.astype(jnp.float32)


def shard_levels(rng, dims, split, least, high):
    def one(dim, blocks):
        draws = jax.random.uniform(jax.random.fold_in(jax.random.fold_in(rng, 6), dim), (blocks,), jnp.float32, least / len(split), high / len(split))
        return jnp.repeat(jnp.exp(draws), dims[dim] // blocks).reshape((-1,) + (1,) * (len(dims) - dim - 1))

    gain = one(*split[0])
    for cut in split[1:]:
        gain = gain * one(*cut)
    return gain


def centred(rng, extent, scale, limit, shards=(), dtype=jnp.bfloat16):
    array = scale * jax.random.normal(rng, extent, jnp.float32)
    if shards:
        array = array * shard_levels(rng, extent, shards, -0.22, 0.18)
    return jnp.clip(array, -limit, limit).astype(dtype)


def setup_inputs(seed: int = 0) -> dict:
    seeds = jax.random.split(jax.random.key(seed), 3)
    return {
        "panel": draw_panel(jax.random.fold_in(seeds[2], 71), 0),
        "rhs": centred(seeds[1], (ROW_CLASSES, RT_DEV * TB, RHS), 1.0, 6.0, ((0, 16),), jnp.float32),
    }


def reference(panel, rhs):
    window = STEPS * TB
    full_panel = panel.reshape(ROW_CLASSES, RT_DEV, TB, COL_CLASSES, CT_DEV, TB)
    full_panel = full_panel.transpose(1, 0, 2, 4, 3, 5).reshape(ORDER, window)
    right_side = rhs.reshape(ROW_CLASSES, RT_DEV, TB, RHS).transpose(1, 0, 2, 3).reshape(ORDER, RHS)
    solved = lax.linalg.triangular_solve(full_panel[:window], right_side[:window], left_side=True, lower=True)
    remainder = right_side - jnp.dot(full_panel.astype(jnp.float32), solved.astype(jnp.float32), precision=lax.Precision.HIGHEST, preferred_element_type=jnp.float32)
    laid_out = remainder.reshape(RT_DEV, ROW_CLASSES, TB, RHS).transpose(1, 0, 2, 3).reshape(ROW_CLASSES, RT_DEV * TB, RHS)
    solved_out = solved.reshape(CT_DEV, COL_CLASSES, TB, RHS).transpose(1, 0, 2, 3).reshape(COL_CLASSES, CT_DEV * TB, RHS)
    return (solved_out, laid_out)
```

```python
import jax
import jax.numpy as jnp
from jax import lax
from jax.experimental import pallas as pl
from jax.experimental.pallas import tpu as pltpu
from jax.sharding import PartitionSpec as P

MESH = pl.DeviceIdType.MESH
F32 = jnp.float32
BF16 = jnp.bfloat16

TB = 512
STEPS = 8
RHS = 256
PIECE = 32
CH = 64
NCH = RHS // CH
NB = 8
BR = 1024
SIDE = 4


def split(a):
    high = a.astype(BF16)
    return high, (a - high.astype(F32)).astype(BF16)


def dot_nn(a, b):
    return jnp.dot(a, b, preferred_element_type=F32)


def dot_nt(a, b):
    return lax.dot_general(a, b, (((1,), (1,)), ((), ())), preferred_element_type=F32)


def mul(a, b):
    ah, al = split(a)
    bh, bl = split(b)
    return dot_nn(ah, bh) + (dot_nn(ah, bl) + dot_nn(al, bh))


def mul_nt(ah, al, bh, bl):
    return dot_nt(ah, bh) + (dot_nt(al, bh) + dot_nt(ah, bl))


def panel_part(full, row, count, part):
    return full[pl.ds(row * 4 + part, count, stride=4), :]


def panel_rows(full, row, count):
    return jnp.concatenate([panel_part(full, row, count, i) for i in range(4)], axis=1)


def permuted(index):
    return index % 2 * 128 + index // 2 * PIECE


def invert_diagonal(full, mh, ml):
    n = 128
    row = lax.broadcasted_iota(jnp.int32, (n, n), 0)
    col = lax.broadcasted_iota(jnp.int32, (n, n), 1)
    inverses = []
    for i in range(4):
        a = panel_part(full, i * n, n, i)
        d = jnp.where(row == col, a, 0.0)
        over_col = 1.0 / jnp.sum(d, axis=1, keepdims=True)
        over_row = 1.0 / jnp.sum(d, axis=0, keepdims=True)
        q = jnp.where(row > col, -a * over_col, 0.0)
        p = q + jnp.where(row == col, 1.0, 0.0)
        q = mul(q, q)
        for step in range(6):
            if step < 5:
                both = mul(q, jnp.concatenate([p, q], axis=1))
                p, q = p + both[:, :n], both[:, n:]
            else:
                p = p + mul(q, p)
        inverses.append(p * over_row)
    wide = []
    zero = jnp.zeros((n, n), F32)
    for i in range(2):
        first, second = inverses[2 * i], inverses[2 * i + 1]
        mid = (2 * i + 1) * n
        low = -mul(second, mul(panel_part(full, mid, n, 2 * i), first))
        wide.append(
            jnp.concatenate(
                [jnp.concatenate([first, zero], 1), jnp.concatenate([low, second], 1)], 0
            )
        )
    corner = jnp.concatenate([panel_part(full, 256, 256, 0), panel_part(full, 256, 256, 1)], 1)
    low = -mul(wide[1], mul(corner, wide[0]))
    for value, r0, c0 in ((wide[0], 0, 0), (low, 256, 0), (wide[1], 256, 256)):
        h, l = split(value)
        mh[r0 : r0 + 256, c0 : c0 + 256] = h
        ml[r0 : r0 + 256, c0 : c0 + 256] = l
    mh[0:256, 256:512] = jnp.zeros((256, 256), BF16)
    ml[0:256, 256:512] = jnp.zeros((256, 256), BF16)


def kernel(
    panel, rhs, x_out, rem_out,
    full, btile, btp, bown, mh, ml, xbuf, xh, xl, sin, sout, pt, d2, ra, fb,
    load_sem, xs, xr, ss, sr, d2s, d2r, as_, ar, bs, cs, fr,
):
    r = lax.axis_index("row")
    c = lax.axis_index("col")
    z, x = r // SIDE, r % SIDE
    y, core = c // 2, c % 2

    def load(i):
        if i == 0:
            return pltpu.make_async_copy(panel.at[pl.ds(0, 4 * TB)], full.at[pl.ds(0, 4 * TB)], load_sem.at[0])
        if i == 1:
            return pltpu.make_async_copy(rhs.at[pl.ds(0, TB)], btile, load_sem.at[1])
        if i == 2:
            rest = pl.ds(4 * TB, 4 * (NB * BR - TB))
            return pltpu.make_async_copy(panel.at[rest], full.at[rest], load_sem.at[2])
        lanes = pl.ds(pl.multiple_of(c // 4 * 128, 128), 128)
        return pltpu.make_async_copy(rhs.at[:, lanes], bown, load_sem.at[3])

    for i in range(4):
        load(i).start()

    def wrap(v):
        return (v + SIDE) % SIDE

    x_peers = (
        (z * SIDE + wrap(x + 1), c),
        (z * SIDE + wrap(x - 1), c),
        (wrap(z + 1) * SIDE + x, c),
        (wrap(z - 1) * SIDE + x, c),
    )
    partner = (r, y * 2 + 1 - core)

    def y_peer(step):
        return (r, wrap(y + step) * 2 + core)

    diagonal = (r, wrap(y + 2 * core - 1) * 2 + 1 - core)

    barrier = pltpu.get_barrier_semaphore()
    for peer in (*x_peers, partner, y_peer(1), y_peer(-1), diagonal):
        pl.semaphore_signal(barrier, inc=1, device_id=peer, device_id_type=MESH)
    pl.semaphore_wait(barrier, 8)

    dx = wrap(x - c % SIDE)
    dz = wrap(z - c // SIDE)
    has_child = (
        jnp.logical_and(dz == 0, dx <= 1),
        jnp.logical_and(dz == 0, dx == 0),
        dz <= 1,
        dz == 0,
    )
    is_diag = r == c
    is_left = jnp.logical_and(r < STEPS, c < r)

    def chunk(k):
        return pl.ds(pl.multiple_of(k * CH, CH), CH)

    def x_copy(j, k):
        return pltpu.make_async_remote_copy(
            src_ref=xbuf.at[chunk(k)], dst_ref=xbuf.at[chunk(k)],
            send_sem=xs.at[j, k], recv_sem=xr.at[k],
            device_id=x_peers[j], device_id_type=MESH,
        )

    def forward(k):
        for j in range(4):
            @pl.when(has_child[j])
            def _():
                x_copy(j, k).start()

    next_col = (r, (c + 1) % STEPS)

    def s_copy(k):
        return pltpu.make_async_remote_copy(
            src_ref=sout.at[chunk(k)], dst_ref=sin.at[chunk(k)],
            send_sem=ss.at[k], recv_sem=sr.at[k],
            device_id=next_col, device_id_type=MESH,
        )

    @pl.when(c == 0)
    def _():
        sin[...] = jnp.zeros_like(sin)

    load(0).wait()
    load(1).wait()

    @pl.when(is_diag)
    def _():
        turned = btile[...].T
        for i in range(STEPS):
            btp[permuted(i) : permuted(i) + PIECE] = turned[i * PIECE : (i + 1) * PIECE]
        invert_diagonal(full, mh, ml)

        def body(k, carry):
            @pl.when(c > 0)
            def _():
                s_copy(k).wait_recv()
            ah, al = split(btp[chunk(k)] - sin[chunk(k)])
            xbuf[chunk(k)] = mul_nt(ah, al, mh[...], ml[...])
            forward(k)
            return carry

        lax.fori_loop(0, NCH, body, 0)

    @pl.when(is_left)
    def _():
        h, l = split(panel_rows(full, 0, TB))
        mh[...] = h
        ml[...] = l

        def body(k, carry):
            x_copy(0, k).wait_recv()
            forward(k)
            ah, al = split(xbuf[chunk(k)])
            product = mul_nt(ah, al, mh[...], ml[...])

            @pl.when(c > 0)
            def _():
                s_copy(k).wait_recv()
            sout[chunk(k)] = product + sin[chunk(k)]
            s_copy(k).start()
            return carry

        lax.fori_loop(0, NCH, body, 0)

    @pl.when(jnp.logical_not(jnp.logical_or(is_diag, is_left)))
    def _():
        def body(k, carry):
            x_copy(0, k).wait_recv()
            forward(k)
            return carry

        lax.fori_loop(0, NCH, body, 0)

    h, l = split(xbuf[...])
    xh[...] = h
    xl[...] = l
    load(2).wait()

    mine = core * 128

    def rows_of(dest):
        return pl.ds(pl.multiple_of(mine + dest * PIECE, PIECE), PIECE)

    def d2_copy(t):
        return pltpu.make_async_remote_copy(
            src_ref=pt.at[t, pl.ds(pl.multiple_of(128 - mine, 128), 128)], dst_ref=d2.at[t],
            send_sem=d2s.at[t], recv_sem=d2r.at[t],
            device_id=partner, device_id_type=MESH,
        )

    def a_copy(t, way):
        return pltpu.make_async_remote_copy(
            src_ref=pt.at[t, rows_of(wrap(y + 2))], dst_ref=ra.at[t],
            send_sem=as_.at[t], recv_sem=ar.at[t],
            device_id=y_peer(way), device_id_type=MESH,
        )

    def b_copy(t, side, way):
        return pltpu.make_async_remote_copy(
            src_ref=pt.at[t, rows_of(wrap(y - way))], dst_ref=fb.at[1 - side, t],
            send_sem=bs.at[t], recv_sem=fr.at[1 - side, t],
            device_id=y_peer(-way), device_id_type=MESH,
        )

    def c_copy(t, side, way):
        return pltpu.make_async_remote_copy(
            src_ref=pt.at[t, rows_of(wrap(y + way))], dst_ref=fb.at[side, t],
            send_sem=cs.at[t], recv_sem=fr.at[side, t],
            device_id=y_peer(way), device_id_type=MESH,
        )

    def place(t):
        side, i = t % 2, t // 2
        return side, 1 - 2 * side, pl.multiple_of((side * 4 + i) * BR, BR)

    def produce(t):
        side, way, base = place(t)
        for q in range(BR // 256):
            bh, bl = split(panel_rows(full, base + q * 256, 256))
            pt[t, :, q * 256 : (q + 1) * 256] = mul_nt(xh[...], xl[...], bh, bl)
        d2_copy(t).start()

    def first_sends(t):
        side, way, base = place(t)
        d2_copy(t).wait_recv()
        own = pl.ds(pl.multiple_of(mine, 128), 128)
        pt[t, own] += d2[t]
        a_copy(t, way).start()
        b_copy(t, side, way).start()

    produce(0)

    def stage_one(t, carry):
        produce(t)
        first_sends(t - 1)
        return carry

    lax.fori_loop(1, NB, stage_one, 0)
    first_sends(NB - 1)

    x_out[...] = jnp.concatenate(
        [xbuf[permuted(i) : permuted(i) + PIECE] for i in range(STEPS)], axis=0
    ).T

    def stage_two(t, carry):
        side, way, base = place(t)
        a_copy(t, way).wait_recv()
        pt[t, rows_of(wrap(y + way))] += ra[t]
        c_copy(t, side, way).start()
        return carry

    lax.fori_loop(0, NB, stage_two, 0)

    load(3).wait()

    def stage_three(t, carry):
        side, way, base = place(t)
        c_copy(t, 0, way).wait_recv()
        c_copy(t, 1, way).wait_recv()
        turned = bown[pl.ds(base, BR)].T
        total = pt[t, rows_of(y)] + fb[0, t] + fb[1, t]
        quarter = c % 4
        chosen = turned[0:PIECE]
        for i in range(1, 4):
            chosen = jnp.where(quarter == i, turned[i * PIECE : (i + 1) * PIECE], chosen)
        rem_out[:, pl.ds(base, BR)] = chosen - total
        return carry

    lax.fori_loop(0, NB, stage_three, 0)

    def drain(t, carry):
        d2_copy(t).wait_send()
        a_copy(t, 1).wait_send()
        b_copy(t, 0, 1).wait_send()
        c_copy(t, 0, 1).wait_send()
        return carry

    lax.fori_loop(0, NB, drain, 0)

    def drain_solve(k, carry):
        for j in range(4):
            @pl.when(has_child[j])
            def _():
                x_copy(j, k).wait_send()

        @pl.when(is_left)
        def _():
            s_copy(k).wait_send()
        return carry

    lax.fori_loop(0, NCH, drain_solve, 0)


def on_device(panel, rhs):
    rows = panel.shape[1]
    panel = panel.reshape(4 * rows, 128)
    rhs = rhs.reshape(rhs.shape[1], rhs.shape[2])
    dma = pltpu.SemaphoreType.DMA
    solved, rest = pl.pallas_call(
        kernel,
        out_shape=(
            jax.ShapeDtypeStruct((TB, RHS), F32),
            jax.ShapeDtypeStruct((PIECE, rows), F32),
        ),
        in_specs=[pl.BlockSpec(memory_space=pl.ANY)] * 2,
        out_specs=(pl.BlockSpec(memory_space=pltpu.VMEM),) * 2,
        scratch_shapes=[
            pltpu.VMEM((4 * rows, 128), F32),
            pltpu.VMEM((TB, RHS), F32),
            pltpu.VMEM((RHS, TB), F32),
            pltpu.VMEM((rows, 128), F32),
            pltpu.VMEM((TB, TB), BF16),
            pltpu.VMEM((TB, TB), BF16),
            pltpu.VMEM((RHS, TB), F32),
            pltpu.VMEM((RHS, TB), BF16),
            pltpu.VMEM((RHS, TB), BF16),
            pltpu.VMEM((RHS, TB), F32),
            pltpu.VMEM((RHS, TB), F32),
            pltpu.VMEM((NB, RHS, BR), F32),
            pltpu.VMEM((NB, 128, BR), F32),
            pltpu.VMEM((NB, PIECE, BR), F32),
            pltpu.VMEM((2, NB, PIECE, BR), F32),
            dma((4,)),
            dma((4, NCH)), dma((NCH,)),
            dma((NCH,)), dma((NCH,)),
            dma((NB,)), dma((NB,)),
            dma((NB,)), dma((NB,)),
            dma((NB,)), dma((NB,)),
            dma((2, NB)),
        ],
        compiler_params=pltpu.CompilerParams(
            collective_id=0, has_side_effects=True, vmem_limit_bytes=60 * 2**20
        ),
        cost_estimate=pl.CostEstimate(
            flops=3 * 2 * rows * TB * RHS, bytes_accessed=24 * 2**20, transcendentals=0
        ),
    )(panel, rhs)
    return (solved[None], rest.T[None])


def solution(mesh):
    return jax.shard_map(
        on_device,
        mesh=mesh,
        in_specs=(P("row", None, "col", None), P("row", None, None)),
        out_specs=(P("col", None, None), P("row", None, "col")),
        check_vma=False,
    )
```

```python
import jax
import jax.numpy as jnp
from jax import lax
from jax.experimental import pallas as pl
from jax.experimental.pallas import tpu as pltpu
from jax.sharding import PartitionSpec as P

MESH = pl.DeviceIdType.MESH
F32 = jnp.float32
BF16 = jnp.bfloat16

TB = 512
STEPS = 8
RHS = 256
PIECE = 32
CH = 16
NCH = RHS // CH
NG = 1
GR = RHS // NG
GP = PIECE // NG
NBK = 8
BC = 8192 // NBK
NT = NG * NBK
SIDE = 4


def split(a):
    high = a.astype(BF16)
    return high, (a - high.astype(F32)).astype(BF16)


def dot_nn(a, b):
    return jnp.dot(a, b, preferred_element_type=F32)


def dot_nt(a, b):
    return lax.dot_general(a, b, (((1,), (1,)), ((), ())), preferred_element_type=F32)


def mul(a, b):
    ah, al = split(a)
    bh, bl = split(b)
    return dot_nn(ah, bh) + (dot_nn(ah, bl) + dot_nn(al, bh))


def mul_nt(stacked, bh, bl):
    n = stacked.shape[0] // 2
    both = dot_nt(stacked, bh)
    return both[:n] + (both[n:] + dot_nt(stacked[:n], bl))


def stack(a):
    return jnp.concatenate(split(a), axis=0)


def panel_part(full, row, count, part):
    return full[pl.ds(row * 4 + part, count, stride=4), :]


def panel_rows(full, row, count):
    return jnp.concatenate([panel_part(full, row, count, i) for i in range(4)], axis=1)


def permuted(device, group):
    return group * GR + device % 2 * (GR // 2) + device // 2 * GP


def invert_diagonal(full, mh, ml):
    n = 128
    row = lax.broadcasted_iota(jnp.int32, (n, n), 0)
    col = lax.broadcasted_iota(jnp.int32, (n, n), 1)
    inverses = []
    for i in range(4):
        a = panel_part(full, i * n, n, i)
        d = jnp.where(row == col, a, 0.0)
        over_col = 1.0 / jnp.sum(d, axis=1, keepdims=True)
        over_row = 1.0 / jnp.sum(d, axis=0, keepdims=True)
        q = jnp.where(row > col, -a * over_col, 0.0)
        p = q + jnp.where(row == col, 1.0, 0.0)
        q = mul(q, q)
        for step in range(6):
            if step < 5:
                both = mul(q, jnp.concatenate([p, q], axis=1))
                p, q = p + both[:, :n], both[:, n:]
            else:
                p = p + mul(q, p)
        inverses.append(p * over_row)
    wide = []
    zero = jnp.zeros((n, n), F32)
    for i in range(2):
        first, second = inverses[2 * i], inverses[2 * i + 1]
        mid = (2 * i + 1) * n
        low = -mul(second, mul(panel_part(full, mid, n, 2 * i), first))
        wide.append(
            jnp.concatenate(
                [jnp.concatenate([first, zero], 1), jnp.concatenate([low, second], 1)], 0
            )
        )
    corner = jnp.concatenate([panel_part(full, 256, 256, 0), panel_part(full, 256, 256, 1)], 1)
    low = -mul(wide[1], mul(corner, wide[0]))
    for value, r0, c0 in ((wide[0], 0, 0), (low, 256, 0), (wide[1], 256, 256)):
        h, l = split(value)
        mh[r0 : r0 + 256, c0 : c0 + 256] = h
        ml[r0 : r0 + 256, c0 : c0 + 256] = l
    mh[0:256, 256:512] = jnp.zeros((256, 256), BF16)
    ml[0:256, 256:512] = jnp.zeros((256, 256), BF16)


def kernel(
    panel, rhs, x_out, rem_out,
    full, lh, ll, btile, btp, bown, bturn, mh, ml, xbuf, x2, sin, sout, pt, d2, ra, fb,
    load_sem, xs, xr, ss, sr, d2s, d2r, as_, ar, bs, cs, fr,
):
    r = lax.axis_index("row")
    c = lax.axis_index("col")
    z, x = r // SIDE, r % SIDE
    y, core = c // 2, c % 2
    rows = NBK * BC

    def load(i):
        if i == 0:
            return pltpu.make_async_copy(panel.at[pl.ds(0, 4 * TB)], full.at[pl.ds(0, 4 * TB)], load_sem.at[0])
        if i == 1:
            return pltpu.make_async_copy(rhs.at[pl.ds(0, TB)], btile, load_sem.at[1])
        if i == 2:
            rest = pl.ds(4 * TB, 4 * (rows - TB))
            return pltpu.make_async_copy(panel.at[rest], full.at[rest], load_sem.at[2])
        lanes = pl.ds(pl.multiple_of(c // 4 * 128, 128), 128)
        return pltpu.make_async_copy(rhs.at[:, lanes], bown, load_sem.at[3])

    load(0).start()
    load(1).start()

    def wrap(v):
        return (v + SIDE) % SIDE

    x_peers = (
        (z * SIDE + wrap(x + 1), c),
        (z * SIDE + wrap(x - 1), c),
        (wrap(z + 1) * SIDE + x, c),
        (wrap(z - 1) * SIDE + x, c),
    )
    partner = (r, y * 2 + 1 - core)

    def y_peer(step):
        return (r, wrap(y + step) * 2 + core)

    diagonal = (r, wrap(y + 2 * core - 1) * 2 + 1 - core)

    barrier = pltpu.get_barrier_semaphore()
    for peer in (*x_peers, partner, y_peer(1), y_peer(-1), diagonal):
        pl.semaphore_signal(barrier, inc=1, device_id=peer, device_id_type=MESH)
    pl.semaphore_wait(barrier, 8)

    dx = wrap(x - c % SIDE)
    dz = wrap(z - c // SIDE)

    def along(d):
        up = jnp.logical_or(d == 0, jnp.logical_and(d == 1, core == 1))
        down = jnp.logical_or(d == 0, jnp.logical_and(d == 3, core == 0))
        return up, down

    def has_child(j, k):
        if j < 2:
            return jnp.logical_and(along(dx)[j], jnp.logical_or(dz == 0, k % 2 == 1))
        return jnp.logical_and(along(dz)[j - 2], jnp.logical_or(dx == 0, k % 2 == 0))

    is_diag = r == c
    is_left = jnp.logical_and(r < STEPS, c < r)
    ahead = jnp.logical_or(jnp.logical_or(is_left, is_diag), c < STEPS - 2)
    passes = jnp.logical_not(jnp.logical_or(is_left, is_diag))

    def chunk(k):
        return pl.ds(pl.multiple_of(k * CH, CH), CH)

    def x_copy(j, k):
        return pltpu.make_async_remote_copy(
            src_ref=xbuf.at[chunk(k)], dst_ref=xbuf.at[chunk(k)],
            send_sem=xs.at[j, k], recv_sem=xr.at[k],
            device_id=x_peers[j], device_id_type=MESH,
        )

    def forward(k):
        for j in range(4):
            @pl.when(has_child(j, k))
            def _():
                x_copy(j, k).start()

    next_col = (r, (c + 1) % STEPS)

    def s_copy(k):
        return pltpu.make_async_remote_copy(
            src_ref=sout.at[chunk(k)], dst_ref=sin.at[chunk(k)],
            send_sem=ss.at[k], recv_sem=sr.at[k],
            device_id=next_col, device_id_type=MESH,
        )

    @pl.when(c == 0)
    def _():
        sin[...] = jnp.zeros_like(sin)

    load(0).wait()
    load(1).wait()
    load(2).start()
    load(3).start()

    @pl.when(is_diag)
    def _():
        turned = btile[...].T
        for i in range(STEPS):
            for g in range(NG):
                at = permuted(i, g)
                btp[at : at + GP] = turned[i * PIECE + g * GP : i * PIECE + (g + 1) * GP]
        invert_diagonal(full, mh, ml)

    @pl.when(is_left)
    def _():
        h, l = split(panel_rows(full, 0, TB))
        mh[...] = h
        ml[...] = l

    load(2).wait()
    load(3).wait()

    def prepare():
        def body(i, carry):
            at = pl.multiple_of(i * 256, 256)
            h, l = split(panel_rows(full, at, 256))
            lh[pl.ds(at, 256)] = h
            ll[pl.ds(at, 256)] = l
            turned = bown[pl.ds(at, 256)].T
            quarter = c % 4
            chosen = turned[0:PIECE]
            for j in range(1, 4):
                chosen = jnp.where(quarter == j, turned[j * PIECE : (j + 1) * PIECE], chosen)
            bturn[:, pl.ds(at, 256)] = chosen
            return carry

        lax.fori_loop(0, rows // 256, body, 0)

    early = c >= 2

    @pl.when(early)
    def _():
        prepare()

    def own_chunk(k, carry):
        @pl.when(c > 0)
        def _():
            s_copy(k).wait_recv()
        xbuf[chunk(k)] = mul_nt(stack(btp[chunk(k)] - sin[chunk(k)]), mh[...], ml[...])
        forward(k)
        return carry

    def left_chunk(k, carry):
        x_copy(0, k).wait_recv()
        forward(k)
        product = mul_nt(stack(xbuf[chunk(k)]), mh[...], ml[...])

        @pl.when(c > 0)
        def _():
            s_copy(k).wait_recv()
        sout[chunk(k)] = product + sin[chunk(k)]
        s_copy(k).start()
        return carry

    def passed_chunk(k, carry):
        x_copy(0, k).wait_recv()
        forward(k)
        return carry

    @pl.when(is_diag)
    def _():
        lax.fori_loop(0, NCH, own_chunk, 0)

    @pl.when(is_left)
    def _():
        lax.fori_loop(0, NCH, left_chunk, 0)

    @pl.when(jnp.logical_and(passes, ahead))
    def _():
        lax.fori_loop(0, NCH, passed_chunk, 0)

    @pl.when(jnp.logical_not(early))
    def _():
        prepare()

    mine = core * (GR // 2)

    def rows_of(dest):
        return pl.ds(pl.multiple_of(mine + dest * GP, GP), GP)

    def d2_copy(t):
        other = pl.ds(pl.multiple_of(GR // 2 - mine, GR // 2), GR // 2)
        return pltpu.make_async_remote_copy(
            src_ref=pt.at[t, other], dst_ref=d2.at[t],
            send_sem=d2s.at[t], recv_sem=d2r.at[t],
            device_id=partner, device_id_type=MESH,
        )

    def a_copy(t, way):
        return pltpu.make_async_remote_copy(
            src_ref=pt.at[t, rows_of(wrap(y + 2))], dst_ref=ra.at[t],
            send_sem=as_.at[t], recv_sem=ar.at[t],
            device_id=y_peer(way), device_id_type=MESH,
        )

    def b_copy(t, side, way):
        return pltpu.make_async_remote_copy(
            src_ref=pt.at[t, rows_of(wrap(y - way))], dst_ref=fb.at[1 - side, t],
            send_sem=bs.at[t], recv_sem=fr.at[1 - side, t],
            device_id=y_peer(-way), device_id_type=MESH,
        )

    def c_copy(t, side, way):
        return pltpu.make_async_remote_copy(
            src_ref=pt.at[t, rows_of(wrap(y + way))], dst_ref=fb.at[side, t],
            send_sem=cs.at[t], recv_sem=fr.at[side, t],
            device_id=y_peer(way), device_id_type=MESH,
        )

    def place(t):
        side, i = t % 2, t % NBK // 2
        return side, 1 - 2 * side, pl.multiple_of((side * (NBK // 2) + i) * BC, BC)

    def produce(g, t):
        side, way, base = place(t)
        wide = min(BC, 1024)

        def body(q, carry):
            for s in range(wide // 256):
                at = pl.multiple_of(q * wide + s * 256, 256)
                part = pl.ds(base + at, 256)
                pt[t, :, pl.ds(at, 256)] = mul_nt(x2[g], lh[part], ll[part])
            return carry

        lax.fori_loop(0, BC // wide, body, 0)
        d2_copy(t).start()

    def first_sends(t):
        side, way, base = place(t)
        d2_copy(t).wait_recv()
        own = pl.ds(pl.multiple_of(mine, GR // 2), GR // 2)
        pt[t, own] += d2[t]
        a_copy(t, way).start()
        b_copy(t, side, way).start()

    def second_sends(t, carry):
        side, way, base = place(t)
        a_copy(t, way).wait_recv()
        pt[t, rows_of(wrap(y + way))] += ra[t]
        c_copy(t, side, way).start()
        return carry

    def one_group(g, carry):
        per = NCH // NG

        @pl.when(jnp.logical_not(ahead))
        def _():
            lax.fori_loop(g * per, (g + 1) * per, passed_chunk, 0)

        x2[g] = stack(xbuf[pl.ds(pl.multiple_of(g * GR, GR), GR)])
        first = g * NBK
        produce(g, first)

        def stage(i, carry):
            produce(g, first + i)
            first_sends(first + i - 1)
            return carry

        lax.fori_loop(1, NBK, stage, 0)
        first_sends(first + NBK - 1)

        @pl.when(g > 0)
        def _():
            lax.fori_loop(first - NBK, first, second_sends, 0)
        return carry

    lax.fori_loop(0, NG, one_group, 0)
    lax.fori_loop(NT - NBK, NT, second_sends, 0)

    pieces = []
    for i in range(STEPS):
        for g in range(NG):
            pieces.append(xbuf[permuted(i, g) : permuted(i, g) + GP])
    x_out[...] = jnp.concatenate(pieces, axis=0).T

    def finish(t, carry):
        side, way, base = place(t)
        c_copy(t, 0, way).wait_recv()
        c_copy(t, 1, way).wait_recv()
        total = pt[t, rows_of(y)] + fb[0, t] + fb[1, t]
        at = (pl.ds(pl.multiple_of(t // NBK * GP, GP), GP), pl.ds(base, BC))
        rem_out[at] = bturn[at] - total
        return carry

    lax.fori_loop(0, NT, finish, 0)

    def drain(t, carry):
        d2_copy(t).wait_send()
        a_copy(t, 1).wait_send()
        b_copy(t, 0, 1).wait_send()
        c_copy(t, 0, 1).wait_send()
        return carry

    lax.fori_loop(0, NT, drain, 0)

    def drain_solve(k, carry):
        for j in range(4):
            @pl.when(has_child(j, k))
            def _():
                x_copy(j, k).wait_send()

        @pl.when(is_left)
        def _():
            s_copy(k).wait_send()
        return carry

    lax.fori_loop(0, NCH, drain_solve, 0)


def on_device(panel, rhs):
    rows = panel.shape[1]
    panel = panel.reshape(4 * rows, 128)
    rhs = rhs.reshape(rhs.shape[1], rhs.shape[2])
    dma = pltpu.SemaphoreType.DMA
    solved, rest = pl.pallas_call(
        kernel,
        out_shape=(
            jax.ShapeDtypeStruct((TB, RHS), F32),
            jax.ShapeDtypeStruct((PIECE, rows), F32),
        ),
        in_specs=[pl.BlockSpec(memory_space=pl.ANY)] * 2,
        out_specs=(pl.BlockSpec(memory_space=pltpu.VMEM),) * 2,
        scratch_shapes=[
            pltpu.VMEM((4 * rows, 128), F32),
            pltpu.VMEM((rows, TB), BF16),
            pltpu.VMEM((rows, TB), BF16),
            pltpu.VMEM((TB, RHS), F32),
            pltpu.VMEM((RHS, TB), F32),
            pltpu.VMEM((rows, 128), F32),
            pltpu.VMEM((PIECE, rows), F32),
            pltpu.VMEM((TB, TB), BF16),
            pltpu.VMEM((TB, TB), BF16),
            pltpu.VMEM((RHS, TB), F32),
            pltpu.VMEM((NG, 2 * GR, TB), BF16),
            pltpu.VMEM((RHS, TB), F32),
            pltpu.VMEM((RHS, TB), F32),
            pltpu.VMEM((NT, GR, BC), F32),
            pltpu.VMEM((NT, GR // 2, BC), F32),
            pltpu.VMEM((NT, GP, BC), F32),
            pltpu.VMEM((2, NT, GP, BC), F32),
            dma((4,)),
            dma((4, NCH)), dma((NCH,)),
            dma((NCH,)), dma((NCH,)),
            dma((NT,)), dma((NT,)),
            dma((NT,)), dma((NT,)),
            dma((NT,)), dma((NT,)),
            dma((2, NT)),
        ],
        compiler_params=pltpu.CompilerParams(
            collective_id=0, has_side_effects=True, vmem_limit_bytes=63 * 2**20
        ),
        cost_estimate=pl.CostEstimate(
            flops=3 * 2 * rows * TB * RHS, bytes_accessed=24 * 2**20, transcendentals=0
        ),
    )(panel, rhs)
    return (solved[None], rest.T[None])


def solution(mesh):
    return jax.shard_map(
        on_device,
        mesh=mesh,
        in_specs=(P("row", None, "col", None), P("row", None, None)),
        out_specs=(P("col", None, None), P("row", None, "col")),
        check_vma=False,
    )
```

```python
import jax
import jax.numpy as jnp
from jax import lax
from jax.experimental import pallas as pl
from jax.experimental.pallas import tpu as pltpu
from jax.sharding import PartitionSpec as P

MESH = pl.DeviceIdType.MESH
F32 = jnp.float32
BF16 = jnp.bfloat16

TB = 512
STEPS = 8
RHS = 256
PIECE = 32
CH = 16
NCH = RHS // CH
NG = 1
GR = RHS // NG
GP = PIECE // NG
NBK = 8
BC = 8192 // NBK
NT = NG * NBK
SIDE = 4


def split(a):
    high = a.astype(BF16)
    return high, (a - high.astype(F32)).astype(BF16)


def dot_nn(a, b):
    return jnp.dot(a, b, preferred_element_type=F32)


def dot_nt(a, b):
    return lax.dot_general(a, b, (((1,), (1,)), ((), ())), preferred_element_type=F32)


def mul(a, b):
    bh, bl = split(b)
    stacked = stack(a)
    n = a.shape[0]
    both = dot_nn(stacked, bh)
    return both[:n] + (both[n:] + dot_nn(stacked[:n], bl))


def mul_once(a, b):
    return dot_nn(a.astype(BF16), b.astype(BF16))


def mul_nt(stacked, bh, bl):
    n = stacked.shape[0] // 2
    both = dot_nt(stacked, bh)
    return both[:n] + (both[n:] + dot_nt(stacked[:n], bl))


def stack(a):
    return jnp.concatenate(split(a), axis=0)


def panel_part(full, row, count, part):
    return full[pl.ds(row * 4 + part, count, stride=4), :]


def panel_rows(full, row, count):
    return jnp.concatenate([panel_part(full, row, count, i) for i in range(4)], axis=1)


def permuted(device, group):
    return group * GR + device % 2 * (GR // 2) + device // 2 * GP


def invert_diagonal(full, mh, ml):
    n = 128
    row = lax.broadcasted_iota(jnp.int32, (n, n), 0)
    col = lax.broadcasted_iota(jnp.int32, (n, n), 1)
    inverses = []
    for i in range(4):
        a = panel_part(full, i * n, n, i)
        d = jnp.where(row == col, a, 0.0)
        over_col = 1.0 / jnp.sum(d, axis=1, keepdims=True)
        over_row = 1.0 / jnp.sum(d, axis=0, keepdims=True)
        q = jnp.where(row > col, -a * over_col, 0.0)
        p = q + jnp.where(row == col, 1.0, 0.0)
        q = mul(q, q)
        for step in range(6):
            if step < 5:
                both = (mul if step < 3 else mul_once)(q, jnp.concatenate([p, q], axis=1))
                p, q = p + both[:, :n], both[:, n:]
            else:
                p = p + mul_once(q, p)
        inverses.append(p * over_row)
    wide = []
    zero = jnp.zeros((n, n), F32)
    for i in range(2):
        first, second = inverses[2 * i], inverses[2 * i + 1]
        mid = (2 * i + 1) * n
        low = -mul(second, mul(panel_part(full, mid, n, 2 * i), first))
        wide.append(
            jnp.concatenate(
                [jnp.concatenate([first, zero], 1), jnp.concatenate([low, second], 1)], 0
            )
        )
    corner = jnp.concatenate([panel_part(full, 256, 256, 0), panel_part(full, 256, 256, 1)], 1)
    low = -mul(wide[1], mul(corner, wide[0]))
    for value, r0, c0 in ((wide[0], 0, 0), (low, 256, 0), (wide[1], 256, 256)):
        h, l = split(value)
        mh[r0 : r0 + 256, c0 : c0 + 256] = h
        ml[r0 : r0 + 256, c0 : c0 + 256] = l
    mh[0:256, 256:512] = jnp.zeros((256, 256), BF16)
    ml[0:256, 256:512] = jnp.zeros((256, 256), BF16)


def kernel(
    panel, rhs, x_out, rem_out,
    full, lh, ll, btile, btp, bown, bturn, mh, ml, xbuf, x2, sin, sout, pt, d2, ra, fb,
    load_sem, xs, xr, ss, sr, d2s, d2r, as_, ar, bs, cs, fr,
):
    r = lax.axis_index("row")
    c = lax.axis_index("col")
    z, x = r // SIDE, r % SIDE
    y, core = c // 2, c % 2
    rows = NBK * BC

    def load(i):
        if i == 0:
            return pltpu.make_async_copy(panel.at[pl.ds(0, 4 * TB)], full.at[pl.ds(0, 4 * TB)], load_sem.at[0])
        if i == 1:
            return pltpu.make_async_copy(rhs.at[pl.ds(0, TB)], btile, load_sem.at[1])
        if i == 2:
            rest = pl.ds(4 * TB, 4 * (rows - TB))
            return pltpu.make_async_copy(panel.at[rest], full.at[rest], load_sem.at[2])
        lanes = pl.ds(pl.multiple_of(c // 4 * 128, 128), 128)
        return pltpu.make_async_copy(rhs.at[:, lanes], bown, load_sem.at[3])

    load(0).start()
    load(1).start()

    def wrap(v):
        return (v + SIDE) % SIDE

    x_peers = (
        (z * SIDE + wrap(x + 1), c),
        (z * SIDE + wrap(x - 1), c),
        (wrap(z + 1) * SIDE + x, c),
        (wrap(z - 1) * SIDE + x, c),
    )
    partner = (r, y * 2 + 1 - core)

    def y_peer(step):
        return (r, wrap(y + step) * 2 + core)

    diagonal = (r, wrap(y + 2 * core - 1) * 2 + 1 - core)

    barrier = pltpu.get_barrier_semaphore()
    for peer in (*x_peers, partner, y_peer(1), y_peer(-1), diagonal):
        pl.semaphore_signal(barrier, inc=1, device_id=peer, device_id_type=MESH)

    dx = wrap(x - c % SIDE)
    dz = wrap(z - c // SIDE)

    def along(d):
        up = jnp.logical_or(d == 0, jnp.logical_and(d == 1, core == 1))
        down = jnp.logical_or(d == 0, jnp.logical_and(d == 3, core == 0))
        return up, down

    def has_child(j, k):
        if j < 2:
            return jnp.logical_and(along(dx)[j], jnp.logical_or(dz == 0, k % 2 == 1))
        return jnp.logical_and(along(dz)[j - 2], jnp.logical_or(dx == 0, k % 2 == 0))

    is_diag = r == c
    is_left = jnp.logical_and(r < STEPS, c < r)
    ahead = jnp.logical_or(jnp.logical_or(is_left, is_diag), c < STEPS - 2)
    passes = jnp.logical_not(jnp.logical_or(is_left, is_diag))

    def chunk(k):
        return pl.ds(pl.multiple_of(k * CH, CH), CH)

    def x_copy(j, k):
        return pltpu.make_async_remote_copy(
            src_ref=xbuf.at[chunk(k)], dst_ref=xbuf.at[chunk(k)],
            send_sem=xs.at[j, k], recv_sem=xr.at[k],
            device_id=x_peers[j], device_id_type=MESH,
        )

    def forward(k):
        for j in range(4):
            @pl.when(has_child(j, k))
            def _():
                x_copy(j, k).start()

    next_col = (r, (c + 1) % STEPS)

    def s_copy(k):
        return pltpu.make_async_remote_copy(
            src_ref=sout.at[chunk(k)], dst_ref=sin.at[chunk(k)],
            send_sem=ss.at[k], recv_sem=sr.at[k],
            device_id=next_col, device_id_type=MESH,
        )

    @pl.when(c == 0)
    def _():
        sin[...] = jnp.zeros_like(sin)

    load(0).wait()
    load(1).wait()
    load(2).start()
    load(3).start()

    @pl.when(is_diag)
    def _():
        turned = btile[...].T
        for i in range(STEPS):
            for g in range(NG):
                at = permuted(i, g)
                btp[at : at + GP] = turned[i * PIECE + g * GP : i * PIECE + (g + 1) * GP]
        invert_diagonal(full, mh, ml)

    @pl.when(is_left)
    def _():
        h, l = split(panel_rows(full, 0, TB))
        mh[...] = h
        ml[...] = l

    pl.semaphore_wait(barrier, 8)

    def prepare():
        load(2).wait()
        load(3).wait()

        def body(i, carry):
            at = pl.multiple_of(i * 256, 256)
            h, l = split(panel_rows(full, at, 256))
            lh[pl.ds(at, 256)] = h
            ll[pl.ds(at, 256)] = l
            turned = bown[pl.ds(at, 256)].T
            quarter = c % 4
            chosen = turned[0:PIECE]
            for j in range(1, 4):
                chosen = jnp.where(quarter == j, turned[j * PIECE : (j + 1) * PIECE], chosen)
            bturn[:, pl.ds(at, 256)] = chosen
            return carry

        lax.fori_loop(0, rows // 256, body, 0)

    early = c >= 2

    @pl.when(early)
    def _():
        prepare()

    def own_chunk(k, carry):
        @pl.when(c > 0)
        def _():
            s_copy(k).wait_recv()
        xbuf[chunk(k)] = mul_nt(stack(btp[chunk(k)] - sin[chunk(k)]), mh[...], ml[...])
        forward(k)
        return carry

    def left_chunk(k, carry):
        x_copy(0, k).wait_recv()
        forward(k)
        product = mul_nt(stack(xbuf[chunk(k)]), mh[...], ml[...])

        @pl.when(c > 0)
        def _():
            s_copy(k).wait_recv()
        sout[chunk(k)] = product + sin[chunk(k)]
        s_copy(k).start()
        return carry

    def passed_chunk(k, carry):
        x_copy(0, k).wait_recv()
        forward(k)
        return carry

    @pl.when(is_diag)
    def _():
        lax.fori_loop(0, NCH, own_chunk, 0)

    @pl.when(is_left)
    def _():
        lax.fori_loop(0, NCH, left_chunk, 0)

    @pl.when(jnp.logical_and(passes, ahead))
    def _():
        lax.fori_loop(0, NCH, passed_chunk, 0)

    @pl.when(jnp.logical_not(early))
    def _():
        prepare()

    mine = core * (GR // 2)

    def rows_of(dest):
        return pl.ds(pl.multiple_of(mine + dest * GP, GP), GP)

    def d2_copy(t):
        other = pl.ds(pl.multiple_of(GR // 2 - mine, GR // 2), GR // 2)
        return pltpu.make_async_remote_copy(
            src_ref=pt.at[t, other], dst_ref=d2.at[t],
            send_sem=d2s.at[t], recv_sem=d2r.at[t],
            device_id=partner, device_id_type=MESH,
        )

    def a_copy(t, way):
        return pltpu.make_async_remote_copy(
            src_ref=pt.at[t, rows_of(wrap(y + 2))], dst_ref=ra.at[t],
            send_sem=as_.at[t], recv_sem=ar.at[t],
            device_id=y_peer(way), device_id_type=MESH,
        )

    def b_copy(t, side, way):
        return pltpu.make_async_remote_copy(
            src_ref=pt.at[t, rows_of(wrap(y - way))], dst_ref=fb.at[1 - side, t],
            send_sem=bs.at[t], recv_sem=fr.at[1 - side, t],
            device_id=y_peer(-way), device_id_type=MESH,
        )

    def c_copy(t, side, way):
        return pltpu.make_async_remote_copy(
            src_ref=pt.at[t, rows_of(wrap(y + way))], dst_ref=fb.at[side, t],
            send_sem=cs.at[t], recv_sem=fr.at[side, t],
            device_id=y_peer(way), device_id_type=MESH,
        )

    def place(t):
        side, i = t % 2, t % NBK // 2
        return side, 1 - 2 * side, pl.multiple_of((side * (NBK // 2) + i) * BC, BC)

    def produce(g, t):
        side, way, base = place(t)
        wide = min(BC, 1024)

        def body(q, carry):
            for s in range(wide // 256):
                at = pl.multiple_of(q * wide + s * 256, 256)
                part = pl.ds(base + at, 256)
                pt[t, :, pl.ds(at, 256)] = mul_nt(x2[g], lh[part], ll[part])
            return carry

        lax.fori_loop(0, BC // wide, body, 0)
        d2_copy(t).start()

    def first_sends(t):
        side, way, base = place(t)
        d2_copy(t).wait_recv()
        own = pl.ds(pl.multiple_of(mine, GR // 2), GR // 2)
        pt[t, own] += d2[t]
        a_copy(t, way).start()
        b_copy(t, side, way).start()

    def second_sends(t, carry):
        side, way, base = place(t)
        a_copy(t, way).wait_recv()
        pt[t, rows_of(wrap(y + way))] += ra[t]
        c_copy(t, side, way).start()
        return carry

    def one_group(g, carry):
        per = NCH // NG

        @pl.when(jnp.logical_not(ahead))
        def _():
            lax.fori_loop(g * per, (g + 1) * per, passed_chunk, 0)

        x2[g] = stack(xbuf[pl.ds(pl.multiple_of(g * GR, GR), GR)])
        first = g * NBK
        produce(g, first)

        def stage(i, carry):
            produce(g, first + i)
            first_sends(first + i - 1)
            return carry

        lax.fori_loop(1, NBK, stage, 0)
        first_sends(first + NBK - 1)

        @pl.when(g > 0)
        def _():
            lax.fori_loop(first - NBK, first, second_sends, 0)
        return carry

    lax.fori_loop(0, NG, one_group, 0)
    lax.fori_loop(NT - NBK, NT, second_sends, 0)

    pieces = []
    for i in range(STEPS):
        for g in range(NG):
            pieces.append(xbuf[permuted(i, g) : permuted(i, g) + GP])
    x_out[...] = jnp.concatenate(pieces, axis=0).T

    def finish(t, carry):
        side, way, base = place(t)
        c_copy(t, 0, way).wait_recv()
        c_copy(t, 1, way).wait_recv()
        total = pt[t, rows_of(y)] + fb[0, t] + fb[1, t]
        at = (pl.ds(pl.multiple_of(t // NBK * GP, GP), GP), pl.ds(base, BC))
        rem_out[at] = bturn[at] - total
        return carry

    lax.fori_loop(0, NT, finish, 0)

    def drain(t, carry):
        d2_copy(t).wait_send()
        a_copy(t, 1).wait_send()
        b_copy(t, 0, 1).wait_send()
        c_copy(t, 0, 1).wait_send()
        return carry

    lax.fori_loop(0, NT, drain, 0)

    def drain_solve(k, carry):
        for j in range(4):
            @pl.when(has_child(j, k))
            def _():
                x_copy(j, k).wait_send()

        @pl.when(is_left)
        def _():
            s_copy(k).wait_send()
        return carry

    lax.fori_loop(0, NCH, drain_solve, 0)


def on_device(panel, rhs):
    rows = panel.shape[1]
    panel = panel.reshape(4 * rows, 128)
    rhs = rhs.reshape(rhs.shape[1], rhs.shape[2])
    dma = pltpu.SemaphoreType.DMA
    solved, rest = pl.pallas_call(
        kernel,
        out_shape=(
            pltpu.VMEM((TB, RHS), F32),
            pltpu.VMEM((PIECE, rows), F32),
        ),
        in_specs=[pl.BlockSpec(memory_space=pl.ANY)] * 2,
        out_specs=(pl.BlockSpec(memory_space=pltpu.VMEM),) * 2,
        scratch_shapes=[
            pltpu.VMEM((4 * rows, 128), F32),
            pltpu.VMEM((rows, TB), BF16),
            pltpu.VMEM((rows, TB), BF16),
            pltpu.VMEM((TB, RHS), F32),
            pltpu.VMEM((RHS, TB), F32),
            pltpu.VMEM((rows, 128), F32),
            pltpu.VMEM((PIECE, rows), F32),
            pltpu.VMEM((TB, TB), BF16),
            pltpu.VMEM((TB, TB), BF16),
            pltpu.VMEM((RHS, TB), F32),
            pltpu.VMEM((NG, 2 * GR, TB), BF16),
            pltpu.VMEM((RHS, TB), F32),
            pltpu.VMEM((RHS, TB), F32),
            pltpu.VMEM((NT, GR, BC), F32),
            pltpu.VMEM((NT, GR // 2, BC), F32),
            pltpu.VMEM((NT, GP, BC), F32),
            pltpu.VMEM((2, NT, GP, BC), F32),
            dma((4,)),
            dma((4, NCH)), dma((NCH,)),
            dma((NCH,)), dma((NCH,)),
            dma((NT,)), dma((NT,)),
            dma((NT,)), dma((NT,)),
            dma((NT,)), dma((NT,)),
            dma((2, NT)),
        ],
        compiler_params=pltpu.CompilerParams(
            collective_id=0, has_side_effects=True, vmem_limit_bytes=60 * 2**20
        ),
        cost_estimate=pl.CostEstimate(
            flops=3 * 2 * rows * TB * RHS, bytes_accessed=24 * 2**20, transcendentals=0
        ),
    )(panel, rhs)
    return (solved[None], rest.T[None])


def solution(mesh):
    return jax.shard_map(
        on_device,
        mesh=mesh,
        in_specs=(P("row", None, "col", None), P("row", None, None)),
        out_specs=(P("col", None, None), P("row", None, "col")),
        check_vma=False,
    )
```

```python
import functools

import jax
import jax.numpy as jnp
from jax import lax
from jax.experimental import pallas as pl
from jax.experimental.pallas import tpu as pltpu
from jax.sharding import PartitionSpec as P

MESH = pl.DeviceIdType.MESH
F32 = jnp.float32
BF16 = jnp.bfloat16

TB = 512
STEPS = 8
RHS = 256
PIECE = 32
CH = 16
NCH = RHS // CH
NG = 1
GR = RHS // NG
GP = PIECE // NG
NBK = 16
BC = 8192 // NBK
NT = NG * NBK
SIDE = 4


def split(a):
    high = a.astype(BF16)
    return high, (a - high.astype(F32)).astype(BF16)


def dot_nn(a, b):
    return jnp.dot(a, b, preferred_element_type=F32)


def dot_nt(a, b):
    return lax.dot_general(a, b, (((1,), (1,)), ((), ())), preferred_element_type=F32)


def mul(a, b):
    bh, bl = split(b)
    stacked = stack(a)
    n = a.shape[0]
    both = dot_nn(stacked, bh)
    return both[:n] + (both[n:] + dot_nn(stacked[:n], bl))


def mul_once(a, b):
    return dot_nn(a.astype(BF16), b.astype(BF16))


def mul_nt(stacked, bh, bl):
    n = stacked.shape[0] // 2
    both = dot_nt(stacked, bh)
    return both[:n] + (both[n:] + dot_nt(stacked[:n], bl))


def stack(a):
    return jnp.concatenate(split(a), axis=0)


def panel_part(full, row, count, part):
    return full[pl.ds(row * 4 + part, count, stride=4), :]


def panel_rows(full, row, count):
    return jnp.concatenate([panel_part(full, row, count, i) for i in range(4)], axis=1)


def permuted(device, group):
    return group * GR + device % 2 * (GR // 2) + device // 2 * GP


def invert_diagonal(full, mh, ml):
    n = 128
    row = lax.broadcasted_iota(jnp.int32, (n, n), 0)
    col = lax.broadcasted_iota(jnp.int32, (n, n), 1)
    inverses = []
    for i in range(4):
        a = panel_part(full, i * n, n, i)
        d = jnp.where(row == col, a, 0.0)
        over_col = 1.0 / jnp.sum(d, axis=1, keepdims=True)
        over_row = 1.0 / jnp.sum(d, axis=0, keepdims=True)
        q = jnp.where(row > col, -a * over_col, 0.0)
        p = q + jnp.where(row == col, 1.0, 0.0)
        q = mul(q, q)
        for step in range(6):
            if step < 5:
                both = (mul if step < 3 else mul_once)(q, jnp.concatenate([p, q], axis=1))
                p, q = p + both[:, :n], both[:, n:]
            else:
                p = p + mul_once(q, p)
        inverses.append(p * over_row)
    wide = []
    zero = jnp.zeros((n, n), F32)
    for i in range(2):
        first, second = inverses[2 * i], inverses[2 * i + 1]
        mid = (2 * i + 1) * n
        low = -mul(second, mul(panel_part(full, mid, n, 2 * i), first))
        wide.append(
            jnp.concatenate(
                [jnp.concatenate([first, zero], 1), jnp.concatenate([low, second], 1)], 0
            )
        )
    corner = jnp.concatenate([panel_part(full, 256, 256, 0), panel_part(full, 256, 256, 1)], 1)
    low = -mul(wide[1], mul(corner, wide[0]))
    for value, r0, c0 in ((wide[0], 0, 0), (low, 256, 0), (wide[1], 256, 256)):
        h, l = split(value)
        mh[r0 : r0 + 256, c0 : c0 + 256] = h
        ml[r0 : r0 + 256, c0 : c0 + 256] = l
    mh[0:256, 256:512] = jnp.zeros((256, 256), BF16)
    ml[0:256, 256:512] = jnp.zeros((256, 256), BF16)


def kernel(
    panel, rhs, x_out, rem_out,
    full, lh, ll, btile, btp, bown, bturn, mh, ml, xbuf, x2, sin, sout, pt, d2, ra, fb,
    load_sem, xs, xr, ss, sr, d2s, d2r, as_, ar, bs, cs, fr,
):
    r = lax.axis_index("row")
    c = lax.axis_index("col")
    z, x = r // SIDE, r % SIDE
    y, core = c // 2, c % 2
    rows = NBK * BC

    def load(i):
        if i == 0:
            return pltpu.make_async_copy(panel.at[pl.ds(0, 4 * TB)], full.at[pl.ds(0, 4 * TB)], load_sem.at[0])
        if i == 1:
            return pltpu.make_async_copy(rhs.at[pl.ds(0, TB)], btile, load_sem.at[1])
        if i == 2:
            rest = pl.ds(4 * TB, 4 * (rows - TB))
            return pltpu.make_async_copy(panel.at[rest], full.at[rest], load_sem.at[2])
        lanes = pl.ds(pl.multiple_of(c // 4 * 128, 128), 128)
        return pltpu.make_async_copy(rhs.at[:, lanes], bown, load_sem.at[3])

    load(0).start()
    load(1).start()

    def wrap(v):
        return (v + SIDE) % SIDE

    x_peers = (
        (z * SIDE + wrap(x + 1), c),
        (z * SIDE + wrap(x - 1), c),
        (wrap(z + 1) * SIDE + x, c),
        (wrap(z - 1) * SIDE + x, c),
    )
    partner = (r, y * 2 + 1 - core)

    def y_peer(step):
        return (r, wrap(y + step) * 2 + core)

    diagonal = (r, wrap(y + 2 * core - 1) * 2 + 1 - core)

    barrier = pltpu.get_barrier_semaphore()
    for peer in (*x_peers, partner, y_peer(1), y_peer(-1), diagonal):
        pl.semaphore_signal(barrier, inc=1, device_id=peer, device_id_type=MESH)

    dx = wrap(x - c % SIDE)
    dz = wrap(z - c // SIDE)

    def along(d):
        up = jnp.logical_or(d == 0, jnp.logical_and(d == 1, core == 1))
        down = jnp.logical_or(d == 0, jnp.logical_and(d == 3, core == 0))
        return up, down

    def has_child(j, k):
        if j < 2:
            return jnp.logical_and(along(dx)[j], jnp.logical_or(dz == 0, k % 2 == 1))
        return jnp.logical_and(along(dz)[j - 2], jnp.logical_or(dx == 0, k % 2 == 0))

    is_diag = r == c
    is_left = jnp.logical_and(r < STEPS, c < r)
    ahead = jnp.logical_or(jnp.logical_or(is_left, is_diag), c < STEPS - 2)
    passes = jnp.logical_not(jnp.logical_or(is_left, is_diag))

    def chunk(k):
        return pl.ds(pl.multiple_of(k * CH, CH), CH)

    def x_copy(j, k):
        return pltpu.make_async_remote_copy(
            src_ref=xbuf.at[chunk(k)], dst_ref=xbuf.at[chunk(k)],
            send_sem=xs.at[j, k], recv_sem=xr.at[k],
            device_id=x_peers[j], device_id_type=MESH,
        )

    def forward(k):
        for j in range(4):
            @pl.when(has_child(j, k))
            def _():
                x_copy(j, k).start()

    next_col = (r, (c + 1) % STEPS)

    def s_copy(k):
        return pltpu.make_async_remote_copy(
            src_ref=sout.at[chunk(k)], dst_ref=sin.at[chunk(k)],
            send_sem=ss.at[k], recv_sem=sr.at[k],
            device_id=next_col, device_id_type=MESH,
        )

    @pl.when(c == 0)
    def _():
        sin[...] = jnp.zeros_like(sin)

    load(0).wait()
    load(1).wait()
    load(2).start()
    load(3).start()

    @pl.when(is_diag)
    def _():
        turned = btile[...].T
        for i in range(STEPS):
            for g in range(NG):
                at = permuted(i, g)
                btp[at : at + GP] = turned[i * PIECE + g * GP : i * PIECE + (g + 1) * GP]
        invert_diagonal(full, mh, ml)

    @pl.when(is_left)
    def _():
        h, l = split(panel_rows(full, 0, TB))
        mh[...] = h
        ml[...] = l

    pl.semaphore_wait(barrier, 8)

    def prepare():
        load(2).wait()
        load(3).wait()

        def body(i, carry):
            at = pl.multiple_of(i * 256, 256)
            h, l = split(panel_rows(full, at, 256))
            lh[pl.ds(at, 256)] = h
            ll[pl.ds(at, 256)] = l
            turned = bown[pl.ds(at, 256)].T
            quarter = c % 4
            chosen = turned[0:PIECE]
            for j in range(1, 4):
                chosen = jnp.where(quarter == j, turned[j * PIECE : (j + 1) * PIECE], chosen)
            bturn[:, pl.ds(at, 256)] = chosen
            return carry

        lax.fori_loop(0, rows // 256, body, 0)

    early = c >= 2

    @pl.when(early)
    def _():
        prepare()

    def own_chunk(k, carry):
        @pl.when(c > 0)
        def _():
            s_copy(k).wait_recv()
        xbuf[chunk(k)] = mul_nt(stack(btp[chunk(k)] - sin[chunk(k)]), mh[...], ml[...])
        forward(k)
        return carry

    def left_chunk(k, carry):
        x_copy(0, k).wait_recv()
        forward(k)
        product = mul_nt(stack(xbuf[chunk(k)]), mh[...], ml[...])

        @pl.when(c > 0)
        def _():
            s_copy(k).wait_recv()
        sout[chunk(k)] = product + sin[chunk(k)]
        s_copy(k).start()
        return carry

    def passed_chunk(k, carry):
        x_copy(0, k).wait_recv()
        forward(k)
        return carry

    @pl.when(is_diag)
    def _():
        lax.fori_loop(0, NCH, own_chunk, 0)

    @pl.when(is_left)
    def _():
        lax.fori_loop(0, NCH, left_chunk, 0)

    @pl.when(jnp.logical_and(passes, ahead))
    def _():
        lax.fori_loop(0, NCH, passed_chunk, 0)

    @pl.when(jnp.logical_not(early))
    def _():
        prepare()

    mine = core * (GR // 2)

    def rows_of(dest):
        return pl.ds(pl.multiple_of(mine + dest * GP, GP), GP)

    def d2_copy(t):
        other = pl.ds(pl.multiple_of(GR // 2 - mine, GR // 2), GR // 2)
        return pltpu.make_async_remote_copy(
            src_ref=pt.at[t, other], dst_ref=d2.at[t],
            send_sem=d2s.at[t], recv_sem=d2r.at[t],
            device_id=partner, device_id_type=MESH,
        )

    def a_copy(t, way):
        return pltpu.make_async_remote_copy(
            src_ref=pt.at[t, rows_of(wrap(y + 2))], dst_ref=ra.at[t],
            send_sem=as_.at[t], recv_sem=ar.at[t],
            device_id=y_peer(way), device_id_type=MESH,
        )

    def b_copy(t, side, way):
        return pltpu.make_async_remote_copy(
            src_ref=pt.at[t, rows_of(wrap(y - way))], dst_ref=fb.at[1 - side, t],
            send_sem=bs.at[t], recv_sem=fr.at[1 - side, t],
            device_id=y_peer(-way), device_id_type=MESH,
        )

    def c_copy(t, side, way):
        return pltpu.make_async_remote_copy(
            src_ref=pt.at[t, rows_of(wrap(y + way))], dst_ref=fb.at[side, t],
            send_sem=cs.at[t], recv_sem=fr.at[side, t],
            device_id=y_peer(way), device_id_type=MESH,
        )

    def place(t):
        side, i = t % 2, t % NBK // 2
        return side, 1 - 2 * side, pl.multiple_of((side * (NBK // 2) + i) * BC, BC)

    def produce(g, t):
        side, way, base = place(t)
        wide = min(BC, 1024)

        def body(q, carry):
            for s in range(wide // 256):
                at = pl.multiple_of(q * wide + s * 256, 256)
                part = pl.ds(base + at, 256)
                pt[t, :, pl.ds(at, 256)] = mul_nt(x2[g], lh[part], ll[part])
            return carry

        lax.fori_loop(0, BC // wide, body, 0)
        d2_copy(t).start()

    def first_sends(t):
        side, way, base = place(t)
        d2_copy(t).wait_recv()
        own = pl.ds(pl.multiple_of(mine, GR // 2), GR // 2)
        pt[t, own] += d2[t]
        a_copy(t, way).start()
        b_copy(t, side, way).start()

    def second_sends(t, carry):
        side, way, base = place(t)
        a_copy(t, way).wait_recv()
        pt[t, rows_of(wrap(y + way))] += ra[t]
        c_copy(t, side, way).start()
        return carry

    def one_group(g, carry):
        per = NCH // NG

        @pl.when(jnp.logical_not(ahead))
        def _():
            lax.fori_loop(g * per, (g + 1) * per, passed_chunk, 0)

        x2[g] = stack(xbuf[pl.ds(pl.multiple_of(g * GR, GR), GR)])
        first = g * NBK
        produce(g, first)

        def stage(i, carry):
            produce(g, first + i)
            first_sends(first + i - 1)
            return carry

        lax.fori_loop(1, NBK, stage, 0)
        first_sends(first + NBK - 1)

        @pl.when(g > 0)
        def _():
            lax.fori_loop(first - NBK, first, second_sends, 0)
        return carry

    lax.fori_loop(0, NG, one_group, 0)
    lax.fori_loop(NT - NBK, NT, second_sends, 0)

    pieces = []
    for i in range(STEPS):
        for g in range(NG):
            pieces.append(xbuf[permuted(i, g) : permuted(i, g) + GP])
    x_out[...] = jnp.concatenate(pieces, axis=0).T

    def finish(t, carry):
        side, way, base = place(t)
        c_copy(t, 0, way).wait_recv()
        c_copy(t, 1, way).wait_recv()
        total = pt[t, rows_of(y)] + fb[0, t] + fb[1, t]
        at = (pl.ds(pl.multiple_of(t // NBK * GP, GP), GP), pl.ds(base, BC))
        rem_out[at] = bturn[at] - total
        return carry

    lax.fori_loop(0, NT, finish, 0)

    def drain(t, carry):
        d2_copy(t).wait_send()
        a_copy(t, 1).wait_send()
        b_copy(t, 0, 1).wait_send()
        c_copy(t, 0, 1).wait_send()
        return carry

    lax.fori_loop(0, NT, drain, 0)

    def drain_solve(k, carry):
        for j in range(4):
            @pl.when(has_child(j, k))
            def _():
                x_copy(j, k).wait_send()

        @pl.when(is_left)
        def _():
            s_copy(k).wait_send()
        return carry

    lax.fori_loop(0, NCH, drain_solve, 0)


def hand_over(solved, rest, solved_out, rest_out, sem):
    copies = (
        pltpu.make_async_copy(solved, solved_out, sem.at[0]),
        pltpu.make_async_copy(rest, rest_out, sem.at[1]),
    )
    for copy in copies:
        copy.start()
    for copy in copies:
        copy.wait()


def on_device(panel, rhs):
    rows = panel.shape[1]
    panel = panel.reshape(4 * rows, 128)
    rhs = rhs.reshape(rhs.shape[1], rhs.shape[2])
    dma = pltpu.SemaphoreType.DMA
    solved, rest = pl.pallas_call(
        kernel,
        out_shape=(
            pltpu.VMEM((TB, RHS), F32),
            pltpu.VMEM((PIECE, rows), F32),
        ),
        in_specs=[pl.BlockSpec(memory_space=pl.ANY)] * 2,
        out_specs=(pl.BlockSpec(memory_space=pltpu.VMEM),) * 2,
        scratch_shapes=[
            pltpu.VMEM((4 * rows, 128), F32),
            pltpu.VMEM((rows, TB), BF16),
            pltpu.VMEM((rows, TB), BF16),
            pltpu.VMEM((TB, RHS), F32),
            pltpu.VMEM((RHS, TB), F32),
            pltpu.VMEM((rows, 128), F32),
            pltpu.VMEM((PIECE, rows), F32),
            pltpu.VMEM((TB, TB), BF16),
            pltpu.VMEM((TB, TB), BF16),
            pltpu.VMEM((RHS, TB), F32),
            pltpu.VMEM((NG, 2 * GR, TB), BF16),
            pltpu.VMEM((RHS, TB), F32),
            pltpu.VMEM((RHS, TB), F32),
            pltpu.VMEM((NT, GR, BC), F32),
            pltpu.VMEM((NT, GR // 2, BC), F32),
            pltpu.VMEM((NT, GP, BC), F32),
            pltpu.VMEM((2, NT, GP, BC), F32),
            dma((4,)),
            dma((4, NCH)), dma((NCH,)),
            dma((NCH,)), dma((NCH,)),
            dma((NT,)), dma((NT,)),
            dma((NT,)), dma((NT,)),
            dma((NT,)), dma((NT,)),
            dma((2, NT)),
        ],
        compiler_params=pltpu.CompilerParams(
            collective_id=0, has_side_effects=True, vmem_limit_bytes=60 * 2**20
        ),
        cost_estimate=pl.CostEstimate(
            flops=3 * 2 * rows * TB * RHS, bytes_accessed=24 * 2**20, transcendentals=0
        ),
    )(panel, rhs)
    keep = functools.partial(pltpu.with_memory_space_constraint, memory_space=pltpu.VMEM)
    solved, rest = pl.pallas_call(
        hand_over,
        out_shape=(
            jax.ShapeDtypeStruct((TB, RHS), F32),
            jax.ShapeDtypeStruct((PIECE, rows), F32),
        ),
        in_specs=[pl.BlockSpec(memory_space=pltpu.VMEM)] * 2,
        out_specs=(pl.BlockSpec(memory_space=pl.ANY),) * 2,
        scratch_shapes=[dma((2,))],
        compiler_params=pltpu.CompilerParams(vmem_limit_bytes=2**20),
    )(keep(solved), keep(rest))
    return (solved[None], rest.T[None])


def solution(mesh):
    return jax.shard_map(
        on_device,
        mesh=mesh,
        in_specs=(P("row", None, "col", None), P("row", None, None)),
        out_specs=(P("col", None, None), P("row", None, "col")),
        check_vma=False,
    )
```

```python
import functools

import jax
import jax.numpy as jnp
from jax import lax
from jax.experimental import pallas as pl
from jax.experimental.pallas import tpu as pltpu
from jax.sharding import PartitionSpec as P

MESH = pl.DeviceIdType.MESH
F32 = jnp.float32
BF16 = jnp.bfloat16

TB = 512
STEPS = 8
RHS = 256
PIECE = 32
CH = 16
NCH = RHS // CH
NG = 1
GR = RHS // NG
GP = PIECE // NG
NBK = 16
BC = 8192 // NBK
NT = NG * NBK
SIDE = 4


def split(a):
    high = a.astype(BF16)
    return high, (a - high.astype(F32)).astype(BF16)


def dot_nn(a, b):
    return jnp.dot(a, b, preferred_element_type=F32)


def dot_nt(a, b):
    return lax.dot_general(a, b, (((1,), (1,)), ((), ())), preferred_element_type=F32)


def mul(a, b):
    bh, bl = split(b)
    stacked = stack(a)
    n = a.shape[0]
    both = dot_nn(stacked, bh)
    return both[:n] + (both[n:] + dot_nn(stacked[:n], bl))


def mul_once(a, b):
    return dot_nn(a.astype(BF16), b.astype(BF16))


def mul_nt(stacked, bh, bl):
    n = stacked.shape[0] // 2
    both = dot_nt(stacked, bh)
    return both[:n] + (both[n:] + dot_nt(stacked[:n], bl))


def stack(a):
    return jnp.concatenate(split(a), axis=0)


def panel_part(full, row, count, part):
    return full[pl.ds(row * 4 + part, count, stride=4), :]


def panel_rows(full, row, count):
    return jnp.concatenate([panel_part(full, row, count, i) for i in range(4)], axis=1)


def permuted(device, group):
    return group * GR + device % 2 * (GR // 2) + device // 2 * GP


def invert_diagonal(full, mh, ml):
    n = 128
    row = lax.broadcasted_iota(jnp.int32, (n, n), 0)
    col = lax.broadcasted_iota(jnp.int32, (n, n), 1)
    inverses = []
    for i in range(4):
        a = panel_part(full, i * n, n, i)
        d = jnp.where(row == col, a, 0.0)
        over_col = 1.0 / jnp.sum(d, axis=1, keepdims=True)
        over_row = 1.0 / jnp.sum(d, axis=0, keepdims=True)
        q = jnp.where(row > col, -a * over_col, 0.0)
        p = q + jnp.where(row == col, 1.0, 0.0)
        q = mul(q, q)
        for step in range(6):
            if step < 5:
                both = (mul if step < 3 else mul_once)(q, jnp.concatenate([p, q], axis=1))
                p, q = p + both[:, :n], both[:, n:]
            else:
                p = p + mul_once(q, p)
        inverses.append(p * over_row)
    wide = []
    zero = jnp.zeros((n, n), F32)
    for i in range(2):
        first, second = inverses[2 * i], inverses[2 * i + 1]
        mid = (2 * i + 1) * n
        low = -mul(second, mul(panel_part(full, mid, n, 2 * i), first))
        wide.append(
            jnp.concatenate(
                [jnp.concatenate([first, zero], 1), jnp.concatenate([low, second], 1)], 0
            )
        )
    corner = jnp.concatenate([panel_part(full, 256, 256, 0), panel_part(full, 256, 256, 1)], 1)
    low = -mul(wide[1], mul(corner, wide[0]))
    for value, r0, c0 in ((wide[0], 0, 0), (low, 256, 0), (wide[1], 256, 256)):
        h, l = split(value)
        mh[r0 : r0 + 256, c0 : c0 + 256] = h
        ml[r0 : r0 + 256, c0 : c0 + 256] = l
    mh[0:256, 256:512] = jnp.zeros((256, 256), BF16)
    ml[0:256, 256:512] = jnp.zeros((256, 256), BF16)


def kernel(
    panel, rhs, x_out, rem_out,
    full, lh, ll, btile, btp, bown, bturn, mh, ml, xbuf, x2, sin, sout, pt, d2, ra, fb,
    load_sem, xs, xr, ss, sr, d2s, d2r, as_, ar, bs, cs, fr,
):
    r = lax.axis_index("row")
    c = lax.axis_index("col")
    z, x = r // SIDE, r % SIDE
    y, core = c // 2, c % 2
    rows = NBK * BC

    def load(i):
        if i == 0:
            return pltpu.make_async_copy(panel.at[pl.ds(0, 4 * TB)], full.at[pl.ds(0, 4 * TB)], load_sem.at[0])
        if i == 1:
            return pltpu.make_async_copy(rhs.at[pl.ds(0, TB)], btile, load_sem.at[1])
        if i == 2:
            rest = pl.ds(4 * TB, 4 * (rows - TB))
            return pltpu.make_async_copy(panel.at[rest], full.at[rest], load_sem.at[2])
        lanes = pl.ds(pl.multiple_of(c // 4 * 128, 128), 128)
        return pltpu.make_async_copy(rhs.at[:, lanes], bown, load_sem.at[3])

    load(0).start()
    load(1).start()

    def wrap(v):
        return (v + SIDE) % SIDE

    x_peers = (
        (z * SIDE + wrap(x + 1), c),
        (z * SIDE + wrap(x - 1), c),
        (wrap(z + 1) * SIDE + x, c),
        (wrap(z - 1) * SIDE + x, c),
    )
    partner = (r, y * 2 + 1 - core)

    def y_peer(step):
        return (r, wrap(y + step) * 2 + core)

    diagonal = (r, wrap(y + 2 * core - 1) * 2 + 1 - core)

    barrier = pltpu.get_barrier_semaphore()
    for peer in (*x_peers, partner, y_peer(1), y_peer(-1), diagonal):
        pl.semaphore_signal(barrier, inc=1, device_id=peer, device_id_type=MESH)

    dx = wrap(x - c % SIDE)
    dz = wrap(z - c // SIDE)

    def along(d):
        up = jnp.logical_or(d == 0, jnp.logical_and(d == 1, core == 1))
        down = jnp.logical_or(d == 0, jnp.logical_and(d == 3, core == 0))
        return up, down

    def has_child(j, k):
        if j < 2:
            return jnp.logical_and(along(dx)[j], jnp.logical_or(dz == 0, k % 2 == 1))
        return jnp.logical_and(along(dz)[j - 2], jnp.logical_or(dx == 0, k % 2 == 0))

    is_diag = r == c
    is_left = jnp.logical_and(r < STEPS, c < r)
    ahead = jnp.logical_or(jnp.logical_or(is_left, is_diag), c < STEPS - 2)
    passes = jnp.logical_not(jnp.logical_or(is_left, is_diag))

    def chunk(k):
        return pl.ds(pl.multiple_of(k * CH, CH), CH)

    def x_copy(j, k):
        return pltpu.make_async_remote_copy(
            src_ref=xbuf.at[chunk(k)], dst_ref=xbuf.at[chunk(k)],
            send_sem=xs.at[j, k], recv_sem=xr.at[k],
            device_id=x_peers[j], device_id_type=MESH,
        )

    def forward(k):
        for j in range(4):
            @pl.when(has_child(j, k))
            def _():
                x_copy(j, k).start()

    next_col = (r, (c + 1) % STEPS)

    def s_copy(k):
        return pltpu.make_async_remote_copy(
            src_ref=sout.at[chunk(k)], dst_ref=sin.at[chunk(k)],
            send_sem=ss.at[k], recv_sem=sr.at[k],
            device_id=next_col, device_id_type=MESH,
        )

    @pl.when(c == 0)
    def _():
        sin[...] = jnp.zeros_like(sin)

    load(0).wait()
    load(1).wait()
    load(2).start()
    load(3).start()

    @pl.when(is_diag)
    def _():
        turned = btile[...].T
        for i in range(STEPS):
            for g in range(NG):
                at = permuted(i, g)
                btp[at : at + GP] = turned[i * PIECE + g * GP : i * PIECE + (g + 1) * GP]
        invert_diagonal(full, mh, ml)

    @pl.when(is_left)
    def _():
        h, l = split(panel_rows(full, 0, TB))
        mh[...] = h
        ml[...] = l

    pl.semaphore_wait(barrier, 8)

    def prepare():
        load(2).wait()
        load(3).wait()

        def body(i, carry):
            at = pl.multiple_of(i * 256, 256)
            h, l = split(panel_rows(full, at, 256))
            lh[pl.ds(at, 256)] = h
            ll[pl.ds(at, 256)] = l
            turned = bown[pl.ds(at, 256)].T
            quarter = c % 4
            chosen = turned[0:PIECE]
            for j in range(1, 4):
                chosen = jnp.where(quarter == j, turned[j * PIECE : (j + 1) * PIECE], chosen)
            bturn[:, pl.ds(at, 256)] = chosen
            return carry

        lax.fori_loop(0, rows // 256, body, 0)

    early = c >= 2

    @pl.when(early)
    def _():
        prepare()

    def own_chunk(k, carry):
        @pl.when(c > 0)
        def _():
            s_copy(k).wait_recv()
        xbuf[chunk(k)] = mul_nt(stack(btp[chunk(k)] - sin[chunk(k)]), mh[...], ml[...])
        forward(k)
        return carry

    def left_chunk(k, carry):
        x_copy(0, k).wait_recv()
        forward(k)
        product = mul_nt(stack(xbuf[chunk(k)]), mh[...], ml[...])

        @pl.when(c > 0)
        def _():
            s_copy(k).wait_recv()
        sout[chunk(k)] = product + sin[chunk(k)]
        s_copy(k).start()
        return carry

    def passed_chunk(k, carry):
        x_copy(0, k).wait_recv()
        forward(k)
        return carry

    @pl.when(is_diag)
    def _():
        lax.fori_loop(0, NCH, own_chunk, 0)

    @pl.when(is_left)
    def _():
        lax.fori_loop(0, NCH, left_chunk, 0)

    @pl.when(jnp.logical_and(passes, ahead))
    def _():
        lax.fori_loop(0, NCH, passed_chunk, 0)

    @pl.when(jnp.logical_not(early))
    def _():
        prepare()

    mine = core * (GR // 2)

    def rows_of(dest):
        return pl.ds(pl.multiple_of(mine + dest * GP, GP), GP)

    def d2_copy(t):
        other = pl.ds(pl.multiple_of(GR // 2 - mine, GR // 2), GR // 2)
        return pltpu.make_async_remote_copy(
            src_ref=pt.at[t, other], dst_ref=d2.at[t],
            send_sem=d2s.at[t], recv_sem=d2r.at[t],
            device_id=partner, device_id_type=MESH,
        )

    def a_copy(t, way):
        return pltpu.make_async_remote_copy(
            src_ref=pt.at[t, rows_of(wrap(y + 2))], dst_ref=ra.at[t],
            send_sem=as_.at[t], recv_sem=ar.at[t],
            device_id=y_peer(way), device_id_type=MESH,
        )

    def b_copy(t, side, way):
        return pltpu.make_async_remote_copy(
            src_ref=pt.at[t, rows_of(wrap(y - way))], dst_ref=fb.at[1 - side, t],
            send_sem=bs.at[t], recv_sem=fr.at[1 - side, t],
            device_id=y_peer(-way), device_id_type=MESH,
        )

    def c_copy(t, side, way):
        return pltpu.make_async_remote_copy(
            src_ref=pt.at[t, rows_of(wrap(y + way))], dst_ref=fb.at[side, t],
            send_sem=cs.at[t], recv_sem=fr.at[side, t],
            device_id=y_peer(way), device_id_type=MESH,
        )

    def place(t):
        side, i = t % 2, t % NBK // 2
        return side, 1 - 2 * side, pl.multiple_of((side * (NBK // 2) + i) * BC, BC)

    def produce(g, t):
        side, way, base = place(t)
        wide = min(BC, 1024)

        def body(q, carry):
            for s in range(wide // 256):
                at = pl.multiple_of(q * wide + s * 256, 256)
                part = pl.ds(base + at, 256)
                pt[t, :, pl.ds(at, 256)] = mul_nt(x2[g], lh[part], ll[part])
            return carry

        lax.fori_loop(0, BC // wide, body, 0)
        d2_copy(t).start()

    def first_sends(t):
        side, way, base = place(t)
        d2_copy(t).wait_recv()
        own = pl.ds(pl.multiple_of(mine, GR // 2), GR // 2)
        pt[t, own] += d2[t]
        a_copy(t, way).start()
        b_copy(t, side, way).start()

    def second_sends(t, carry):
        side, way, base = place(t)
        a_copy(t, way).wait_recv()
        pt[t, rows_of(wrap(y + way))] += ra[t]
        c_copy(t, side, way).start()
        return carry

    def one_group(g, carry):
        per = NCH // NG

        @pl.when(jnp.logical_not(ahead))
        def _():
            lax.fori_loop(g * per, (g + 1) * per, passed_chunk, 0)

        x2[g] = stack(xbuf[pl.ds(pl.multiple_of(g * GR, GR), GR)])
        first = g * NBK
        produce(g, first)

        def stage(i, carry):
            produce(g, first + i)
            first_sends(first + i - 1)
            return carry

        lax.fori_loop(1, NBK, stage, 0)
        first_sends(first + NBK - 1)

        @pl.when(g > 0)
        def _():
            lax.fori_loop(first - NBK, first, second_sends, 0)
        return carry

    lax.fori_loop(0, NG, one_group, 0)
    lax.fori_loop(NT - NBK, NT, second_sends, 0)

    pieces = []
    for i in range(STEPS):
        for g in range(NG):
            pieces.append(xbuf[permuted(i, g) : permuted(i, g) + GP])
    x_out[...] = jnp.concatenate(pieces, axis=0).T

    def finish(t, carry):
        side, way, base = place(t)
        c_copy(t, 0, way).wait_recv()
        c_copy(t, 1, way).wait_recv()
        total = pt[t, rows_of(y)] + fb[0, t] + fb[1, t]
        at = (pl.ds(pl.multiple_of(t // NBK * GP, GP), GP), pl.ds(base, BC))
        rem_out[at] = bturn[at] - total
        return carry

    lax.fori_loop(0, NT, finish, 0)

    def drain(t, carry):
        d2_copy(t).wait_send()
        a_copy(t, 1).wait_send()
        b_copy(t, 0, 1).wait_send()
        c_copy(t, 0, 1).wait_send()
        return carry

    lax.fori_loop(0, NT, drain, 0)

    def drain_solve(k, carry):
        for j in range(4):
            @pl.when(has_child(j, k))
            def _():
                x_copy(j, k).wait_send()

        @pl.when(is_left)
        def _():
            s_copy(k).wait_send()
        return carry

    lax.fori_loop(0, NCH, drain_solve, 0)


def hand_over(solved, rest, solved_out, rest_out, sem):
    copies = (
        pltpu.make_async_copy(solved, solved_out, sem.at[0]),
        pltpu.make_async_copy(rest, rest_out, sem.at[1]),
    )
    for copy in copies:
        copy.start()
    for copy in copies:
        copy.wait()


def on_device(panel, rhs):
    rows = panel.shape[1]
    panel = panel.reshape(4 * rows, 128)
    rhs = rhs.reshape(rhs.shape[1], rhs.shape[2])
    dma = pltpu.SemaphoreType.DMA
    solved, rest = pl.pallas_call(
        kernel,
        out_shape=(
            pltpu.VMEM((TB, RHS), F32),
            pltpu.VMEM((PIECE, rows), F32),
        ),
        in_specs=[pl.BlockSpec(memory_space=pl.ANY)] * 2,
        out_specs=(pl.BlockSpec(memory_space=pltpu.VMEM),) * 2,
        scratch_shapes=[
            pltpu.VMEM((4 * rows + 8, 128), F32),
            pltpu.VMEM((rows, TB), BF16),
            pltpu.VMEM((rows, TB), BF16),
            pltpu.VMEM((TB, RHS), F32),
            pltpu.VMEM((RHS, TB), F32),
            pltpu.VMEM((rows, 128), F32),
            pltpu.VMEM((PIECE, rows), F32),
            pltpu.VMEM((TB, TB), BF16),
            pltpu.VMEM((TB, TB), BF16),
            pltpu.VMEM((RHS, TB), F32),
            pltpu.VMEM((NG, 2 * GR, TB), BF16),
            pltpu.VMEM((RHS, TB), F32),
            pltpu.VMEM((RHS, TB), F32),
            pltpu.VMEM((NT, GR, BC), F32),
            pltpu.VMEM((NT, GR // 2, BC), F32),
            pltpu.VMEM((NT, GP, BC), F32),
            pltpu.VMEM((2, NT, GP, BC), F32),
            dma((4,)),
            dma((4, NCH)), dma((NCH,)),
            dma((NCH,)), dma((NCH,)),
            dma((NT,)), dma((NT,)),
            dma((NT,)), dma((NT,)),
            dma((NT,)), dma((NT,)),
            dma((2, NT)),
        ],
        compiler_params=pltpu.CompilerParams(
            collective_id=0, has_side_effects=True, vmem_limit_bytes=60 * 2**20
        ),
        cost_estimate=pl.CostEstimate(
            flops=3 * 2 * rows * TB * RHS, bytes_accessed=24 * 2**20, transcendentals=0
        ),
    )(panel, rhs)
    keep = functools.partial(pltpu.with_memory_space_constraint, memory_space=pltpu.VMEM)
    solved, rest = pl.pallas_call(
        hand_over,
        out_shape=(
            jax.ShapeDtypeStruct((TB, RHS), F32),
            jax.ShapeDtypeStruct((PIECE, rows), F32),
        ),
        in_specs=[pl.BlockSpec(memory_space=pltpu.VMEM)] * 2,
        out_specs=(pl.BlockSpec(memory_space=pl.ANY),) * 2,
        scratch_shapes=[dma((2,))],
        compiler_params=pltpu.CompilerParams(vmem_limit_bytes=2**20),
    )(keep(solved), keep(rest))
    return (solved[None], rest.T[None])


def solution(mesh):
    return jax.shard_map(
        on_device,
        mesh=mesh,
        in_specs=(P("row", None, "col", None), P("row", None, None)),
        out_specs=(P("col", None, None), P("row", None, "col")),
        check_vma=False,
    )
```
